256 devices in a mesh: grp: 4 (over y, x), freq: 64 (over z, core).
Axes of the slice: x: 2, y: 2, z: 32, core: 2. Of those that a mesh axis runs over, the one named last changes fastest.
The devices are a block of a 4x8x32 slice.
Arguments:
- kernel: bfloat16 [2, 512, 1024, 1024], P(None, ('grp', 'freq')), parts along dimension 1, may hold values from -0.125 to 0.125
- recorded: float32 [2, 512, 1024, 128], P(None, ('grp', 'freq')), parts along dimension 1, may hold values from -8 to 8
- onset_time: int32 [4096, 128], P(('grp', 'freq')), parts along dimension 0, may hold values from 32 to 256, as said below
Outputs:
- focusing: float32 [256, 4096, 128], P(None, ('grp', 'freq')), parts along dimension 1
The draws below stay inside these ranges and needn't reach their ends.
There are 4 independent parts, one for each index of `grp`. The reference program is written for one: setup_inputs(seed, part) draws one part's arguments, and reference() takes and returns one part's arrays. A program takes and returns all parts, laid end to end along the dimension named above; each array names one. Nothing has to cross between parts.
Inputs may be any that keep to these rules, and one draw needn't show every extreme that they name: `onset_time`: onset sample of the window for each receiver and focal point.
All inputs are finite; a program needn't handle non-finite values.
Results may differ from the reference program's by a relative error of at most 0.012.
Values may be sent and summed in bfloat16 or wider, within the bound.
A program may use at most 64 MiB of HBM per device.

```python
import math
import jax
import jax.numpy as jnp
from jax import lax

SRC = 1024
REC = 1024
NF = 128
FOCAL = 128
ITERS = 2
NT = 256


def draw_recorded(key, part):
    shape = (2, NF, SRC, FOCAL)
    base = jax.random.normal(jax.random.fold_in(key, 21), shape, jnp.float32)
    column_log = jax.random.uniform(jax.random.fold_in(key, 22), (1, 1, 1, FOCAL), jnp.float32, -2.5, 1.5)
    tilt = jax.random.uniform(jax.random.fold_in(key, 23), (1, 1, 1, FOCAL), jnp.float32, -2.0, 2.0)
    source_log = jax.random.uniform(jax.random.fold_in(key, 24), (1, 1, SRC, 1), jnp.float32, -0.8, 0.8)
    freq_pos = (jnp.arange(NF, dtype=jnp.float32) / NF - 0.5).reshape(1, NF, 1, 1)
    value = base * jnp.exp(column_log + tilt * freq_pos + source_log)
    return jnp.clip(value, -8.0, 8.0).astype(jnp.float32)


def draw_onset_time(key, part):
    rows = jnp.arange(REC, dtype=jnp.int32)[:, None]
    base = NT // 8 + rows * (5 * NT // 8) // REC
    jitter = jax.random.randint(jax.random.fold_in(key, 11), (REC, FOCAL), 0, NT // 4 + 1, dtype=jnp.int32)
    column_shift = jax.random.randint(jax.random.fold_in(key, 12), (1, FOCAL), -(3 * NT // 8), NT // 2 + 1, dtype=jnp.int32)
    onset = jnp.clip(base + jitter + column_shift, NT // 8, NT).astype(jnp.int32)
    onset = onset.at[0, 0].set(NT // 8)
    onset = onset.at[REC - 1, 0].set(NT)
    return onset.astype(jnp.int32)


def shard_levels(rng, shape, split, least, largest):
    factor_of, own = 1.0, jax.random.fold_in(rng, 6)
    for dim, shards_of in split:
        draws = jnp.exp(jax.random.uniform(jax.random.fold_in(own, dim), (shards_of,), jnp.float32, least / len(split), largest / len(split)))
        factor_of = factor_of * jnp.repeat(draws, shape[dim] // shards_of).reshape([-1 if axis == dim else 1 for axis in range(len(shape))])
    return factor_of


def noise(own_key, extent, width, reach, shards=(), held_as=jnp.bfloat16):
    array = jax.random.normal(own_key, extent, jnp.float32) * width
    if len(shards) > 0:
        array = shard_levels(own_key, extent, shards, -0.22, 0.18) * array
    return jnp.clip(array, min=-reach, max=reach).astype(held_as)


def setup_inputs(seed: int = 0, part: int = 0) -> dict:
    seeds = jax.random.split(jax.random.key(seed), 4)
    part_keys = jax.random.split(jax.random.fold_in(seeds[3], part), 4)
    kernel = noise(part_keys[0], (2, NF, SRC, REC), (2 * REC) ** -0.5, 0.125, ((1, 64),))
    recorded = draw_recorded(jax.random.fold_in(jax.random.fold_in(seeds[3], part), 71), part)
    onset_time = draw_onset_time(jax.random.fold_in(jax.random.fold_in(seeds[3], part), 71), part)
    return {"kernel": kernel, "recorded": recorded, "onset_time": onset_time}


def dft_tables():
    samples = jnp.arange(2 * NF, dtype=jnp.int32)
    bins = jnp.arange(NF, dtype=jnp.int32)
    phase = (bins[:, None] * samples[None, :] % (2 * NF)).astype(jnp.float32) * (math.pi / NF)
    factor = 1.0 / math.sqrt(NF)
    return (jnp.cos(phase) * factor, jnp.sin(phase) * factor)

def reference(kernel, recorded, onset_time):
    highest = lax.Precision.HIGHEST
    cosine_table, sin_tab = dft_tables()
    samples = jnp.arange(2 * NF, dtype=jnp.int32)[:, None, None]
    keep_mask = (samples < onset_time[None]).astype(jnp.float32)
    kern_major = jnp.moveaxis(kernel, 1, 0)

    def apply_forward(model):
        flat_part = (model * keep_mask).reshape(2 * NF, -1)
        spec_real = jnp.dot(cosine_table, flat_part, precision=highest)
        spec_imag = -jnp.dot(sin_tab, flat_part, precision=highest)
        spectrum = jnp.stack([spec_real, spec_imag]).reshape(2, NF, REC, FOCAL).astype(jnp.bfloat16)

        def per_freq(pair):
            kern_slab, spectrum_block = pair
            kernel_real = kern_slab[0].astype(jnp.float32)
            kernel_imaginary = kern_slab[1].astype(jnp.float32)
            solution_real = spectrum_block[0].astype(jnp.float32)
            solution_imaginary = spectrum_block[1].astype(jnp.float32)
            y_real = jnp.dot(kernel_real, solution_real, precision=highest) - jnp.dot(kernel_imaginary, solution_imaginary, precision=highest)
            y_imag = jnp.dot(kernel_real, solution_imaginary, precision=highest) + jnp.dot(kernel_imaginary, solution_real, precision=highest)
            return jnp.stack([y_real, y_imag])
        return jnp.moveaxis(lax.map(per_freq, (kern_major, jnp.moveaxis(spectrum, 1, 0))), 0, 1)

    def apply_adjoint(resid):
        rounded = jnp.moveaxis(resid.astype(jnp.bfloat16), 1, 0)

        def per_freq(pair):
            kern_slab, data_slab = pair
            kernel_real = kern_slab[0].astype(jnp.float32)
            kernel_imaginary = kern_slab[1].astype(jnp.float32)
            update_real = data_slab[0].astype(jnp.float32)
            update_imaginary = data_slab[1].astype(jnp.float32)
            z_real = jnp.dot(kernel_real.T, update_real, precision=highest) + jnp.dot(kernel_imaginary.T, update_imaginary, precision=highest)
            z_imag = jnp.dot(kernel_real.T, update_imaginary, precision=highest) - jnp.dot(kernel_imaginary.T, update_real, precision=highest)
            return jnp.stack([z_real, z_imag]).astype(jnp.bfloat16)
        image_low = lax.optimization_barrier(jnp.moveaxis(lax.map(per_freq, (kern_major, rounded)), 0, 1))
        image = image_low.astype(jnp.float32)
        timed = jnp.dot(cosine_table.T, image[0].reshape(NF, -1), precision=highest) - jnp.dot(sin_tab.T, image[1].reshape(NF, -1), precision=highest)
        return timed.reshape(2 * NF, REC, FOCAL) * keep_mask
    beta_now = jnp.sqrt(jnp.sum(recorded * recorded))
    data_vec = recorded / beta_now
    model_raw = apply_adjoint(data_vec)
    alpha_now = jnp.sqrt(jnp.sum(model_raw * model_raw))
    model_vec = model_raw / alpha_now
    search = model_vec
    estimate = jnp.zeros_like(model_vec)
    phibar_now = beta_now
    rhobar_now = alpha_now
    for iteration in range(ITERS):
        data_raw = apply_forward(model_vec) - alpha_now * data_vec
        beta_now = jnp.sqrt(jnp.sum(data_raw * data_raw))
        data_vec = data_raw / beta_now
        model_raw = apply_adjoint(data_vec) - beta_now * model_vec
        alpha_now = jnp.sqrt(jnp.sum(model_raw * model_raw))
        model_vec = model_raw / alpha_now
        rho_now = jnp.sqrt(rhobar_now * rhobar_now + beta_now * beta_now)
        cosine = rhobar_now / rho_now
        sine_part = beta_now / rho_now
        theta_now = sine_part * alpha_now
        rhobar_now = -cosine * alpha_now
        phi_now = cosine * phibar_now
        phibar_now = sine_part * phibar_now
        estimate = estimate + phi_now / rho_now * search
        search = model_vec - theta_now / rho_now * search
    return estimate
```

```python
import functools

import jax
import jax.numpy as jnp
import numpy as np
from jax import lax
from jax.experimental import pallas as pl
from jax.experimental.pallas import tpu as pltpu
from jax.sharding import PartitionSpec as P

CORES = 2
HALF = 8
MIB = 2**20
MESH = pl.DeviceIdType.MESH
F32 = jnp.float32
BF16 = jnp.bfloat16


def dft_tables(bins):
    samples = 2 * bins
    phase = np.outer(np.arange(bins), np.arange(samples)) % samples * (np.pi / bins)
    scale = 1.0 / np.sqrt(bins)
    both = np.concatenate([np.cos(phase) * scale, -np.sin(phase) * scale], axis=0)
    return both.astype(jnp.bfloat16)


def dot(left, right):
    return jnp.dot(left, right, preferred_element_type=F32)


def body(
    group,
    kern_hbm,
    data_hbm,
    onset,
    to_freq,
    to_time,
    out,
    kern,
    kern_t,
    data,
    resid,
    weights,
    model,
    field,
    image_out,
    image_in,
    spec_out,
    spec_in,
    wide,
    sums_out,
    sums_in,
    load_sem,
    send_sem,
    recv_sem,
    own_sem,
    sum_send,
    sum_recv,
):
    me = lax.axis_index("freq")
    chips = group // CORES
    chip = me // CORES
    core = lax.rem(me, CORES)
    nf = kern.shape[1]
    src = kern.shape[2]
    rec = kern.shape[3]
    focal = onset.shape[1]
    bins = group * nf
    samples = 2 * bins

    def peer(chip_step, core_step):
        return lax.rem(chip + chip_step + chips, chips) * CORES + lax.rem(core + core_step, CORES)

    def for_peers(act):
        far = chips // 2
        for other in range(CORES):
            act(peer(far, other))

        def step(i, carry):
            d = far - 1 - i
            for other in range(CORES):
                act(peer(d, other))
                act(peer(-d, other))
            return carry

        lax.fori_loop(0, far - 1, step, 0)
        act(peer(0, 1))

    barrier = pltpu.get_barrier_semaphore()
    for_peers(
        lambda p: pl.semaphore_signal(barrier, inc=1, device_id={"freq": p}, device_id_type=MESH)
    )
    loads = []
    for h in range(nf):
        for c in range(2):
            loads.append(pltpu.make_async_copy(data_hbm.at[c, h], data.at[c, h], load_sem.at[0, c, h]))
            loads.append(pltpu.make_async_copy(kern_hbm.at[c, h], kern.at[c, h], load_sem.at[1, c, h]))
    for load in loads:
        load.start()

    def exchange(outgoing, incoming, kind, turn, part):
        send = send_sem.at[kind, turn, part]
        recv = recv_sem.at[kind, turn, part]
        source = outgoing.at[turn, part]
        target = incoming.at[turn, part]

        def push(p):
            pltpu.make_async_remote_copy(
                src_ref=source.at[p],
                dst_ref=target.at[me],
                send_sem=send,
                recv_sem=recv,
                device_id={"freq": p},
                device_id_type=MESH,
            ).start()

        for_peers(push)
        pltpu.make_async_copy(source.at[me], target.at[me], own_sem.at[kind, turn, part]).start()

    def arrived(outgoing, incoming, kind, turn, part):
        source = outgoing.at[turn, part]
        target = incoming.at[turn, part]
        rest = target.at[pl.ds(0, group - 1)]
        pltpu.make_async_copy(rest, rest, recv_sem.at[kind, turn, part]).wait()
        pltpu.make_async_copy(source.at[me], target.at[me], own_sem.at[kind, turn, part]).wait()

    def sent(outgoing, kind, turn, part):
        rest = outgoing.at[turn, part, pl.ds(0, group - 1)]
        pltpu.make_async_copy(rest, rest, send_sem.at[kind, turn, part]).wait()

    lane = lax.broadcasted_iota(jnp.int32, (1, 128), 1)

    def share(slot, values):
        row = jnp.zeros((1, 128), F32)
        for i, value in enumerate(values):
            row = jnp.where(lane == i, value, row)
        sums_out[slot] = row
        sums_in[slot, me] = row

        def push(p):
            pltpu.make_async_remote_copy(
                src_ref=sums_out.at[slot],
                dst_ref=sums_in.at[slot, me],
                send_sem=sum_send.at[slot],
                recv_sem=sum_recv.at[slot],
                device_id={"freq": p},
                device_id_type=MESH,
            ).start()

        for_peers(push)

    def collect(slot, count):
        rest = sums_in.at[slot, pl.ds(0, group - 1)]
        pltpu.make_async_copy(rest, rest, sum_recv.at[slot]).wait()
        total = jnp.sum(sums_in[slot], axis=0)
        return [jnp.sum(jnp.where(lane == i, total, 0.0), axis=1, keepdims=True) for i in range(count)]

    def full_sum(values):
        return jnp.sum(jnp.sum(values, axis=0, keepdims=True), axis=1, keepdims=True)

    def put_weights(h, rows, real, imag):
        rows_low = pl.ds(src + rows.start, rows.size)
        weights[h, rows, :focal] = real.astype(BF16)
        weights[h, rows, focal:] = imag.astype(BF16)
        weights[h, rows_low, :focal] = imag.astype(BF16)
        weights[h, rows_low, focal:] = (-real).astype(BF16)

    block = 256

    def adjoint(turn):
        for h in range(nf):

            def step(i, carry):
                rows = pl.ds(pl.multiple_of(i * block, block), block)
                got = dot(kern_t[0, h, rows, :], weights[h, :src, :]) + dot(
                    kern_t[1, h, rows, :], weights[h, src:, :]
                )
                owners = block // (2 * HALF)
                real = got[:, :focal].reshape(owners, 2, HALF, focal)
                imag = got[:, focal:].reshape(owners, 2, HALF, focal)
                for part in range(2):
                    image_out[turn, part, pl.ds(i * owners, owners), h] = jnp.concatenate(
                        [real[:, part], imag[:, part]], axis=1
                    ).astype(BF16)
                return carry

            lax.fori_loop(0, rec // block, step, 0)

    def window(turn, part, combine):
        wide[...] = image_in[turn, part].astype(F32).reshape(bins * 2 * HALF, focal)
        norm = jnp.zeros((1, 2 * focal), F32)
        time = lax.broadcasted_iota(jnp.int32, (samples, focal), 0)
        for pair in range(HALF // 2):
            first, second = 2 * pair, 2 * pair + 1

            def column(r):
                return jnp.concatenate(
                    [
                        wide[pl.ds(r, bins, stride=2 * HALF), :],
                        wide[pl.ds(HALF + r, bins, stride=2 * HALF), :],
                    ],
                    axis=0,
                ).astype(BF16)

            timed = dot(to_time[...], jnp.concatenate([column(first), column(second)], axis=1))
            kept = []
            for i, r in enumerate((first, second)):
                row = part * HALF + r
                keep = time < onset[pl.ds(row, 1), :]
                value = jnp.where(keep, timed[:, i * focal : (i + 1) * focal], 0.0)
                kept.append(combine(row, value))
            kept = jnp.concatenate(kept, axis=1)
            norm = norm + jnp.sum(kept * kept, axis=0, keepdims=True)
            spec = dot(to_freq[...], kept.astype(BF16))
            for i, r in enumerate((first, second)):
                cols = slice(i * focal, (i + 1) * focal)
                wide[pl.ds(r, bins, stride=2 * HALF), :] = spec[:bins, cols]
                wide[pl.ds(HALF + r, bins, stride=2 * HALF), :] = spec[bins:, cols]
        spec_out[turn, part] = wide[...].reshape(group, nf, 2 * HALF, focal).astype(BF16)
        return norm

    def forward(turn, finish):
        norm = jnp.zeros((1, 2 * focal), F32)
        for h in range(nf):

            def spread(i, carry):
                owners = 8
                parts = [
                    spec_in[turn, part, pl.ds(i * owners, owners), h].astype(F32) for part in range(2)
                ]
                rows = pl.ds(pl.multiple_of(i * owners * 2 * HALF, 128), owners * 2 * HALF)
                real = jnp.concatenate([p[:, :HALF] for p in parts], axis=1).reshape(-1, focal)
                imag = jnp.concatenate([p[:, HALF:] for p in parts], axis=1).reshape(-1, focal)
                rows_low = pl.ds(pl.multiple_of(rec + i * owners * 2 * HALF, 128), owners * 2 * HALF)
                weights[h, rows, :focal] = real.astype(BF16)
                weights[h, rows, focal:] = imag.astype(BF16)
                weights[h, rows_low, :focal] = (-imag).astype(BF16)
                weights[h, rows_low, focal:] = real.astype(BF16)
                return carry

            lax.fori_loop(0, group // 8, spread, 0)

            def step(i, norm):
                rows = pl.ds(pl.multiple_of(i * block, block), block)
                got = dot(kern[0, h, rows, :], weights[h, :rec, :]) + dot(
                    kern[1, h, rows, :], weights[h, rec:, :]
                )
                value = finish(h, rows, got)
                return norm + jnp.sum(value * value, axis=0, keepdims=True)

            norm = lax.fori_loop(0, src // block, step, norm)
        return full_sum(norm)

    data_norm = jnp.zeros((1, focal), F32)
    for load in loads[0::2]:
        load.wait()
    for h in range(nf):
        for c in range(2):
            data_norm = data_norm + jnp.sum(data[c, h] * data[c, h], axis=0, keepdims=True)
        put_weights(h, pl.ds(0, src), data[0, h], data[1, h])
    data_norm = full_sum(data_norm)
    for load in loads[1::2]:
        load.wait()
    tile = 256
    for h in range(nf):
        for c in range(2):

            def flip(i, carry):
                cols = pl.ds(pl.multiple_of(i * tile, tile), tile)
                kern_t[c, h, cols, :] = kern[c, h, :, cols].T
                return carry

            lax.fori_loop(0, rec // tile, flip, 0)
    adjoint(0)
    pl.semaphore_wait(barrier, group - 1)
    exchange(image_out, image_in, 0, 0, 0)
    exchange(image_out, image_in, 0, 0, 1)

    norms = []
    for part in range(2):
        arrived(image_out, image_in, 0, 0, part)

        def keep_model(row, value):
            model[row] = value
            return value

        norms.append(window(0, part, keep_model))
        if part == 1:
            share(0, (data_norm, full_sum(norms[0] + norms[1])))
        exchange(spec_out, spec_in, 1, 0, part)

    square_data, square_model = collect(0, 2)
    beta0 = jnp.sqrt(square_data)
    size0 = jnp.sqrt(square_model)
    alpha0 = size0 / beta0
    for part in range(2):
        arrived(spec_out, spec_in, 1, 0, part)
    gain = 1.0 / size0
    back = alpha0 / beta0

    def first_resid(h, rows, got):
        real = got[:, :focal] * gain - back * data[0, h, rows, :]
        imag = got[:, focal:] * gain - back * data[1, h, rows, :]
        value = jnp.concatenate([real, imag], axis=1)
        resid[h, rows, :] = value
        return value

    resid_square = forward(0, first_resid)
    share(1, (resid_square,))

    for h in range(nf):
        put_weights(h, pl.ds(0, src), resid[h, :, :focal], resid[h, :, focal:])
    adjoint(1)
    exchange(image_out, image_in, 0, 1, 0)
    exchange(image_out, image_in, 0, 1, 1)

    (square1,) = collect(1, 1)
    beta1 = jnp.sqrt(square1)
    scale1 = 1.0 / beta1
    back1 = beta1 / size0
    norms = []
    for part in range(2):
        arrived(image_out, image_in, 0, 1, part)

        def subtract(row, value):
            value = value * scale1 - back1 * model[row]
            field[row] = value
            return value

        norms.append(window(1, part, subtract))
        if part == 1:
            share(2, (full_sum(norms[0] + norms[1]),))
        exchange(spec_out, spec_in, 1, 1, part)

    (square2,) = collect(2, 1)
    alpha1 = jnp.sqrt(square2)
    gain2 = 1.0 / alpha1
    back2 = alpha1 / beta1
    for part in range(2):
        arrived(spec_out, spec_in, 1, 1, part)

    def second_resid(h, rows, got):
        return got * gain2 - back2 * resid[h, rows, :]

    last_square = forward(1, second_resid)
    share(3, (last_square,))
    (square3,) = collect(3, 1)
    beta2 = jnp.sqrt(square3)
    rho1 = jnp.sqrt(alpha0 * alpha0 + beta1 * beta1)
    cosine = alpha0 / rho1
    sine = beta1 / rho1
    theta = sine * alpha1
    rhobar = -cosine * alpha1
    phi1 = cosine * beta0
    phibar = sine * beta0
    rho2 = jnp.sqrt(rhobar * rhobar + beta2 * beta2)
    phi2 = rhobar / rho2 * phibar
    step2 = phi2 / rho2
    on_field = step2 / alpha1
    on_model = (phi1 / rho1 - step2 * (theta / rho1)) / size0
    held = onset.shape[0]
    for row in range(held):
        out[pl.ds(row, samples, stride=held), :] = on_model * model[row] + on_field * field[row]

    for turn in range(2):
        for part in range(2):
            sent(image_out, 0, turn, part)
            sent(spec_out, 1, turn, part)
    for slot in range(4):
        rest = sums_in.at[slot, pl.ds(0, group - 1)]
        pltpu.make_async_copy(rest, rest, sum_send.at[slot]).wait()


def solution(mesh):
    group = mesh.shape["freq"]

    def shard(kernel, recorded, onset_time):
        nf, src, rec = kernel.shape[1:]
        held, focal = onset_time.shape
        bins = group * nf
        samples = 2 * bins
        forth = dft_tables(bins)
        moved = (2, 2, group, nf, 2 * HALF, focal)
        dma = pltpu.SemaphoreType.DMA
        x = pl.pallas_call(
            functools.partial(body, group),
            out_shape=jax.ShapeDtypeStruct((samples * held, focal), F32),
            in_specs=[
                pl.BlockSpec(memory_space=pl.ANY),
                pl.BlockSpec(memory_space=pl.ANY),
                pl.BlockSpec(memory_space=pltpu.VMEM),
                pl.BlockSpec(memory_space=pltpu.VMEM),
                pl.BlockSpec(memory_space=pltpu.VMEM),
            ],
            out_specs=pl.BlockSpec(memory_space=pltpu.VMEM),
            scratch_shapes=[
                pltpu.VMEM(kernel.shape, BF16),
                pltpu.VMEM((2, nf, rec, src), BF16),
                pltpu.VMEM(recorded.shape, F32),
                pltpu.VMEM((nf, src, 2 * focal), F32),
                pltpu.VMEM((nf, src + rec, 2 * focal), BF16),
                pltpu.VMEM((held, samples, focal), F32),
                pltpu.VMEM((held, samples, focal), F32),
                pltpu.VMEM(moved, BF16),
                pltpu.VMEM(moved, BF16),
                pltpu.VMEM(moved, BF16),
                pltpu.VMEM(moved, BF16),
                pltpu.VMEM((bins * 2 * HALF, focal), F32),
                pltpu.VMEM((4, 1, 128), F32),
                pltpu.VMEM((4, group, 1, 128), F32),
                dma((2, 2, nf)),
                dma((2, 2, 2)),
                dma((2, 2, 2)),
                dma((2, 2, 2)),
                dma((4,)),
                dma((4,)),
            ],
            compiler_params=pltpu.CompilerParams(
                collective_id=0, has_side_effects=True, vmem_limit_bytes=60 * MIB
            ),
        )(kernel, recorded, onset_time, jnp.asarray(forth), jnp.asarray(np.ascontiguousarray(forth.T)))
        return x.reshape(samples, held, focal)

    placed = (
        P(None, ("grp", "freq"), None, None),
        P(None, ("grp", "freq"), None, None),
        P(("grp", "freq"), None),
    )
    return jax.shard_map(
        shard, mesh=mesh, in_specs=placed, out_specs=P(None, ("grp", "freq"), None), check_vma=False
    )
```

```python
import functools

import jax
import jax.numpy as jnp
import numpy as np
from jax import lax
from jax.experimental import pallas as pl
from jax.experimental.pallas import tpu as pltpu
from jax.sharding import PartitionSpec as P

CORES = 2
HALF = 8
MIB = 2**20
TEAMS = 4
TEAM_ORDER = (2, 1, 3, 0)
LIMIT = 42
MESH = pl.DeviceIdType.MESH
F32 = jnp.float32
BF16 = jnp.bfloat16


def dft_tables(bins):
    samples = 2 * bins
    phase = np.outer(np.arange(bins), np.arange(samples)) % samples * (np.pi / bins)
    scale = 1.0 / np.sqrt(bins)
    both = np.concatenate([np.cos(phase) * scale, -np.sin(phase) * scale], axis=0)
    return both.astype(jnp.bfloat16)


def dot(left, right):
    return jnp.dot(left, right, preferred_element_type=F32)


def body(
    group,
    kern_hbm,
    data_hbm,
    onset,
    to_freq,
    to_time,
    model_hbm,
    field_hbm,
    mix,
    kern,
    kern_t,
    data,
    resid,
    duals,
    weights,
    partial,
    model,
    field,
    image_out,
    image_in,
    spec_out,
    spec_in,
    wide,
    sums_out,
    sums_in,
    data_sem,
    kern_sem,
    send_sem,
    image_sem,
    spec_sem,
    own_sem,
    sum_send,
    sum_recv,
    save_sem,
):
    me = lax.axis_index("freq")
    chips = group // CORES
    chip = me // CORES
    core = lax.rem(me, CORES)
    nf = kern.shape[1]
    src = kern.shape[2]
    focal = onset.shape[1]
    held = onset.shape[0]
    bins = group * nf
    samples = 2 * bins
    team = group // TEAMS
    mine = me // team
    seat = lax.rem(me, team)
    block = team * held
    order = [lax.rem(mine + i, TEAMS) for i in TEAM_ORDER]

    def peer(chip_step, core_step):
        return lax.rem(chip + chip_step + chips, chips) * CORES + lax.rem(core + core_step, CORES)

    def for_peers(act):
        far = chips // 2
        for other in range(CORES):
            act(peer(far, other))

        def step(i, carry):
            d = far - 1 - i
            for other in range(CORES):
                act(peer(d, other))
                act(peer(-d, other))
            return carry

        lax.fori_loop(0, far - 1, step, 0)
        act(peer(0, 1))

    barrier = pltpu.get_barrier_semaphore()
    for_peers(
        lambda p: pl.semaphore_signal(barrier, inc=1, device_id={"freq": p}, device_id_type=MESH)
    )

    def cols_of(t):
        return pl.ds(pl.multiple_of(order[t] * block, block), block)

    def data_load(c, h):
        return pltpu.make_async_copy(data_hbm.at[c, h], data.at[c, h], data_sem.at[c, h])

    def kern_load(t, c, h):
        where = (c, h, slice(None), cols_of(t))
        return pltpu.make_async_copy(kern_hbm.at[where], kern.at[where], kern_sem.at[t, c, h])

    for h in range(nf):
        for c in range(2):
            data_load(c, h).start()
    for t in range(TEAMS):
        for h in range(nf):
            for c in range(2):
                kern_load(t, c, h).start()

    def remote(outgoing, incoming, kind, turn, part, recv, p):
        pltpu.make_async_remote_copy(
            src_ref=outgoing.at[turn, part, p],
            dst_ref=incoming.at[turn, part, me],
            send_sem=send_sem.at[kind, turn, part],
            recv_sem=recv,
            device_id={"freq": p},
            device_id_type=MESH,
        ).start()

    def own(outgoing, incoming, kind, turn, part):
        return pltpu.make_async_copy(
            outgoing.at[turn, part, me], incoming.at[turn, part, me], own_sem.at[kind, turn, part]
        )

    def send_image(turn, part, p):
        remote(image_out, image_in, 0, turn, part, image_sem.at[turn, part], p)

    def image_arrived(turn, part):
        rest = image_in.at[turn, part, pl.ds(0, group - 1)]
        pltpu.make_async_copy(rest, rest, image_sem.at[turn, part]).wait()
        own(image_out, image_in, 0, turn, part).wait()

    def send_spec(turn, part):
        for_peers(
            lambda p: remote(spec_out, spec_in, 1, turn, part, spec_sem.at[turn, part, mine], p)
        )
        own(spec_out, spec_in, 1, turn, part).start()

    def spec_arrived(turn, part, t):
        count = team - 1 if TEAM_ORDER[t] == 0 else team
        rest = spec_in.at[turn, part, pl.ds(0, count)]
        pltpu.make_async_copy(rest, rest, spec_sem.at[turn, part, order[t]]).wait()
        if TEAM_ORDER[t] == 0:
            own(spec_out, spec_in, 1, turn, part).wait()

    def sent(outgoing, kind, turn, part):
        rest = outgoing.at[turn, part, pl.ds(0, group - 1)]
        pltpu.make_async_copy(rest, rest, send_sem.at[kind, turn, part]).wait()

    lane = lax.broadcasted_iota(jnp.int32, (1, 128), 1)

    def row_of(values):
        row = jnp.zeros((1, 128), F32)
        for i, value in enumerate(values):
            row = jnp.where(lane == i, value, row)
        return row

    def share(slot, values):
        row = row_of(values)
        sums_out[slot] = row
        sums_in[slot, me] = row

        def push(p):
            pltpu.make_async_remote_copy(
                src_ref=sums_out.at[slot],
                dst_ref=sums_in.at[slot, me],
                send_sem=sum_send.at[slot],
                recv_sem=sum_recv.at[slot],
                device_id={"freq": p},
                device_id_type=MESH,
            ).start()

        for_peers(push)

    def collect(slot, count):
        rest = sums_in.at[slot, pl.ds(0, group - 1)]
        pltpu.make_async_copy(rest, rest, sum_recv.at[slot]).wait()
        total = jnp.sum(sums_in[slot], axis=0)
        return [jnp.sum(jnp.where(lane == i, total, 0.0), axis=1, keepdims=True) for i in range(count)]

    def full_sum(values):
        return jnp.sum(jnp.sum(values, axis=0, keepdims=True), axis=1, keepdims=True)

    def put_duals(h, rows, real, imag):
        low = pl.ds(pl.multiple_of(src + rows.start, 128), rows.size)
        duals[h, rows, :focal] = real.astype(BF16)
        duals[h, rows, focal:] = imag.astype(BF16)
        duals[h, low, :focal] = imag.astype(BF16)
        duals[h, low, focal:] = (-real).astype(BF16)

    tile = 256

    def adjoint(turn, t, ready):
        rows = cols_of(t)
        owner = order[t] * team
        for h in range(nf):
            ready(t, h)
            got = dot(kern_t[0, h, rows, :], duals[h, :src, :]) + dot(
                kern_t[1, h, rows, :], duals[h, src:, :]
            )
            real = got[:, :focal].reshape(team, 2, HALF, focal)
            imag = got[:, focal:].reshape(team, 2, HALF, focal)
            for part in range(2):
                image_out[turn, part, pl.ds(owner, team), h] = jnp.concatenate(
                    [real[:, part], imag[:, part]], axis=1
                ).astype(BF16)

    def send_team(turn, t):
        first = 1 if TEAM_ORDER[t] == 0 else 0

        def push(i, carry):
            send_image(turn, 0, order[t] * team + lax.rem(seat + i, team))
            return carry

        lax.fori_loop(first, team, push, 0)

    def send_rest(turn):
        own(image_out, image_in, 0, turn, 0).start()
        for_peers(lambda p: send_image(turn, 1, p))
        own(image_out, image_in, 0, turn, 1).start()

    def row_at(row):
        return pl.ds(row, samples, stride=held)

    def window(turn, part, combine):
        wide[...] = image_in[turn, part].astype(F32).reshape(bins * 2 * HALF, focal)
        norm = jnp.zeros((1, 2 * focal), F32)
        time = lax.broadcasted_iota(jnp.int32, (samples, focal), 0)
        for pair in range(HALF // 2):
            first, second = 2 * pair, 2 * pair + 1

            def column(r):
                return jnp.concatenate(
                    [
                        wide[pl.ds(r, bins, stride=2 * HALF), :],
                        wide[pl.ds(HALF + r, bins, stride=2 * HALF), :],
                    ],
                    axis=0,
                ).astype(BF16)

            timed = dot(to_time[...], jnp.concatenate([column(first), column(second)], axis=1))
            kept = []
            for i, r in enumerate((first, second)):
                row = part * HALF + r
                keep = time < onset[pl.ds(row, 1), :]
                value = jnp.where(keep, timed[:, i * focal : (i + 1) * focal], 0.0)
                kept.append(combine(row, value))
            kept = jnp.concatenate(kept, axis=1)
            norm = norm + jnp.sum(kept * kept, axis=0, keepdims=True)
            spec = dot(to_freq[...], kept.astype(BF16))
            for i, r in enumerate((first, second)):
                cols = slice(i * focal, (i + 1) * focal)
                wide[pl.ds(r, bins, stride=2 * HALF), :] = spec[:bins, cols]
                wide[pl.ds(HALF + r, bins, stride=2 * HALF), :] = spec[bins:, cols]
        spec_out[turn, part] = wide[...].reshape(group, nf, 2 * HALF, focal).astype(BF16)
        return norm

    def forward(turn, finish):
        norm = jnp.zeros((1, 2 * focal), F32)
        for t in range(TEAMS):
            for part in range(2):
                spec_arrived(turn, part, t)
            for h in range(nf):
                blocks = [
                    spec_in[turn, part, pl.ds(order[t] * team, team), h].astype(F32)
                    for part in range(2)
                ]
                real = jnp.concatenate([b[:, :HALF] for b in blocks], axis=1).reshape(block, focal)
                imag = jnp.concatenate([b[:, HALF:] for b in blocks], axis=1).reshape(block, focal)
                weights[h, 0, :, :focal] = real.astype(BF16)
                weights[h, 0, :, focal:] = imag.astype(BF16)
                weights[h, 1, :, :focal] = (-imag).astype(BF16)
                weights[h, 1, :, focal:] = real.astype(BF16)

                def step(i, norm):
                    rows = pl.ds(pl.multiple_of(i * tile, tile), tile)
                    got = dot(kern[0, h, rows, cols_of(t)], weights[h, 0]) + dot(
                        kern[1, h, rows, cols_of(t)], weights[h, 1]
                    )
                    if t > 0:
                        got = got + partial[h, rows, :]
                    if t < TEAMS - 1:
                        partial[h, rows, :] = got
                        return norm
                    value = finish(h, rows, got)
                    return norm + jnp.sum(value * value, axis=0, keepdims=True)

                norm = lax.fori_loop(0, src // tile, step, norm)
        return full_sum(norm)

    for h in range(nf):
        for c in range(2):
            data_load(c, h).wait()
        put_duals(h, pl.ds(0, src), data[0, h], data[1, h])

    def turn_block(t, h):
        for c in range(2):
            kern_load(t, c, h).wait()

            def flip(i, carry):
                at = pl.ds(pl.multiple_of(i * tile, tile), tile)
                kern_t[c, h, cols_of(t), at] = kern[c, h, at, cols_of(t)].T
                return carry

            lax.fori_loop(0, src // tile, flip, 0)

    for t in range(TEAMS):
        adjoint(0, t, turn_block)
        if t == 0:
            pl.semaphore_wait(barrier, group - 1)
        send_team(0, t)
    send_rest(0)
    data_norm = jnp.zeros((1, focal), F32)
    for h in range(nf):
        for c in range(2):
            data_norm = data_norm + jnp.sum(data[c, h] * data[c, h], axis=0, keepdims=True)
    data_norm = full_sum(data_norm)

    norms = []
    for part in range(2):
        image_arrived(0, part)

        def keep_model(row, value):
            model[row_at(row), :] = value
            return value

        norms.append(window(0, part, keep_model))
        if part == 1:
            share(0, (data_norm, full_sum(norms[0] + norms[1])))
        send_spec(0, part)
    save_model = pltpu.make_async_copy(model, model_hbm, save_sem.at[0])
    save_model.start()

    square_data, square_model = collect(0, 2)
    beta0 = jnp.sqrt(square_data)
    size0 = jnp.sqrt(square_model)
    alpha0 = size0 / beta0
    gain = 1.0 / size0
    back = alpha0 / beta0

    def first_resid(h, rows, got):
        real = got[:, :focal] * gain - back * data[0, h, rows, :]
        imag = got[:, focal:] * gain - back * data[1, h, rows, :]
        put_duals(h, rows, real, imag)
        value = jnp.concatenate([real, imag], axis=1)
        resid[h, rows, :] = value
        return value

    resid_square = forward(0, first_resid)
    share(1, (resid_square,))
    for t in range(TEAMS):
        adjoint(1, t, lambda t, h: None)
        send_team(1, t)
    send_rest(1)

    (square1,) = collect(1, 1)
    beta1 = jnp.sqrt(square1)
    scale1 = 1.0 / beta1
    back1 = beta1 / size0
    norms = []
    for part in range(2):
        image_arrived(1, part)

        def subtract(row, value):
            value = value * scale1 - back1 * model[row_at(row), :]
            field[row_at(row), :] = value
            return value

        norms.append(window(1, part, subtract))
        if part == 1:
            share(2, (full_sum(norms[0] + norms[1]),))
        send_spec(1, part)
    save_field = pltpu.make_async_copy(field, field_hbm, save_sem.at[1])
    save_field.start()

    (square2,) = collect(2, 1)
    alpha1 = jnp.sqrt(square2)
    gain2 = 1.0 / alpha1
    back2 = alpha1 / beta1

    def second_resid(h, rows, got):
        return got * gain2 - back2 * resid[h, rows, :]

    last_square = forward(1, second_resid)
    share(3, (last_square,))
    save_model.wait()
    save_field.wait()
    for turn in range(2):
        for part in range(2):
            sent(image_out, 0, turn, part)
            sent(spec_out, 1, turn, part)
    for slot in range(4):
        rest = sums_in.at[slot, pl.ds(0, group - 1)]
        pltpu.make_async_copy(rest, rest, sum_send.at[slot]).wait()
    (square3,) = collect(3, 1)
    beta2 = jnp.sqrt(square3)
    rho1 = jnp.sqrt(alpha0 * alpha0 + beta1 * beta1)
    cosine = alpha0 / rho1
    sine = beta1 / rho1
    theta = sine * alpha1
    rhobar = -cosine * alpha1
    phi1 = cosine * beta0
    phibar = sine * beta0
    rho2 = jnp.sqrt(rhobar * rhobar + beta2 * beta2)
    phi2 = rhobar / rho2 * phibar
    step2 = phi2 / rho2
    on_field = step2 / alpha1
    on_model = (phi1 / rho1 - step2 * (theta / rho1)) / size0
    mix[0:1, :] = jnp.broadcast_to(on_model, (1, focal))
    mix[1:2, :] = jnp.broadcast_to(on_field, (1, focal))


def solution(mesh):
    group = mesh.shape["freq"]

    def shard(kernel, recorded, onset_time):
        nf, src, rec = kernel.shape[1:]
        held, focal = onset_time.shape
        bins = group * nf
        samples = 2 * bins
        forth = dft_tables(bins)
        moved = (2, 2, group, nf, 2 * HALF, focal)
        flat = (samples * held, focal)
        dma = pltpu.SemaphoreType.DMA
        vmem = pl.BlockSpec(memory_space=pltpu.VMEM)
        anywhere = pl.BlockSpec(memory_space=pl.ANY)
        model, field, mix = pl.pallas_call(
            functools.partial(body, group),
            out_shape=(
                jax.ShapeDtypeStruct(flat, F32),
                jax.ShapeDtypeStruct(flat, F32),
                jax.ShapeDtypeStruct((2, focal), F32),
            ),
            in_specs=[anywhere, anywhere, vmem, vmem, vmem],
            out_specs=(anywhere, anywhere, vmem),
            scratch_shapes=[
                pltpu.VMEM(kernel.shape, BF16),
                pltpu.VMEM((2, nf, rec, src), BF16),
                pltpu.VMEM(recorded.shape, F32),
                pltpu.VMEM((nf, src, 2 * focal), F32),
                pltpu.VMEM((nf, 2 * src, 2 * focal), BF16),
                pltpu.VMEM((nf, 2, rec // TEAMS, 2 * focal), BF16),
                pltpu.VMEM((nf, src, 2 * focal), F32),
                pltpu.VMEM(flat, F32),
                pltpu.VMEM(flat, F32),
                pltpu.VMEM(moved, BF16),
                pltpu.VMEM(moved, BF16),
                pltpu.VMEM(moved, BF16),
                pltpu.VMEM(moved, BF16),
                pltpu.VMEM((bins * 2 * HALF, focal), F32),
                pltpu.VMEM((4, 1, 128), F32),
                pltpu.VMEM((4, group, 1, 128), F32),
                dma((2, nf)),
                dma((TEAMS, 2, nf)),
                dma((2, 2, 2)),
                dma((2, 2)),
                dma((2, 2, TEAMS)),
                dma((2, 2, 2)),
                dma((4,)),
                dma((4,)),
                dma((2,)),
            ],
            compiler_params=pltpu.CompilerParams(
                collective_id=0, has_side_effects=True, vmem_limit_bytes=LIMIT * MIB
            ),
        )(kernel, recorded, onset_time, jnp.asarray(forth), jnp.asarray(np.ascontiguousarray(forth.T)))
        x = mix[0:1] * model + mix[1:2] * field
        return x.reshape(samples, held, focal)

    placed = (
        P(None, ("grp", "freq"), None, None),
        P(None, ("grp", "freq"), None, None),
        P(("grp", "freq"), None),
    )
    return jax.shard_map(
        shard, mesh=mesh, in_specs=placed, out_specs=P(None, ("grp", "freq"), None), check_vma=False
    )
```

```python
import functools

import jax
import jax.numpy as jnp
import numpy as np
from jax import lax
from jax.experimental import pallas as pl
from jax.experimental.pallas import tpu as pltpu
from jax.sharding import PartitionSpec as P

CORES = 2
HALF = 8
MIB = 2**20
TEAMS = 4
TEAM_ORDER = (2, 1, 3, 0)
LIMIT = 58
TALL = 512
LAST = 3
MESH = pl.DeviceIdType.MESH
F32 = jnp.float32
BF16 = jnp.bfloat16


def dft_tables(bins):
    samples = 2 * bins
    phase = np.outer(np.arange(bins), np.arange(samples)) % samples * (np.pi / bins)
    scale = 1.0 / np.sqrt(bins)
    both = np.concatenate([np.cos(phase) * scale, -np.sin(phase) * scale], axis=0)
    return both.astype(jnp.bfloat16)


def dot(left, right):
    return jnp.dot(left, right, preferred_element_type=F32)


def body(
    group,
    kern_hbm,
    data_hbm,
    onset_hbm,
    to_freq_hbm,
    to_time_hbm,
    model_hbm,
    field_hbm,
    on_model,
    on_field,
    onset,
    to_freq,
    to_time,
    kern,
    kern_t,
    data,
    resid,
    duals,
    weights,
    partial,
    model,
    field,
    image_out,
    image_in,
    spec_out,
    spec_in,
    wide,
    sums_own,
    sums_mate,
    sums_out,
    sums_in,
    last_in,
    small_sem,
    data_sem,
    kern_sem,
    send_sem,
    image_sem,
    spec_sem,
    own_sem,
    mate_send,
    mate_recv,
    sum_send,
    sum_recv,
    save_sem,
):
    me = lax.axis_index("freq")
    chips = group // CORES
    chip = me // CORES
    core = lax.rem(me, CORES)
    nf = kern.shape[1]
    src = kern.shape[2]
    held, focal = onset.shape
    bins = group * nf
    samples = 2 * bins
    team = group // TEAMS
    mine = me // team
    seat = lax.rem(me, team)
    block = team * held
    order = [lax.rem(mine + i, TEAMS) for i in TEAM_ORDER]

    def peer(chip_step, core_step):
        return lax.rem(chip + chip_step + chips, chips) * CORES + lax.rem(core + core_step, CORES)

    def for_peers(act):
        far = chips // 2
        for other in range(CORES):
            act(peer(far, other))

        def step(i, carry):
            d = far - 1 - i
            for other in range(CORES):
                act(peer(d, other))
                act(peer(-d, other))
            return carry

        lax.fori_loop(0, far - 1, step, 0)
        act(peer(0, 1))

    barrier = pltpu.get_barrier_semaphore()
    for_peers(
        lambda p: pl.semaphore_signal(barrier, inc=1, device_id={"freq": p}, device_id_type=MESH)
    )

    def cols_of(t):
        return pl.ds(pl.multiple_of(order[t] * block, block), block)

    def data_load(c, h):
        return pltpu.make_async_copy(data_hbm.at[c, h], data.at[c, h], data_sem.at[c, h])

    def kern_load(t, c, h):
        where = (c, h, slice(None), cols_of(t))
        return pltpu.make_async_copy(kern_hbm.at[where], kern.at[where], kern_sem.at[t, c, h])

    for h in range(nf):
        for c in range(2):
            data_load(c, h).start()
    for t in range(TEAMS):
        for h in range(nf):
            for c in range(2):
                kern_load(t, c, h).start()
    small = [
        pltpu.make_async_copy(source, target, small_sem.at[i])
        for i, (source, target) in enumerate(
            ((onset_hbm, onset), (to_freq_hbm, to_freq), (to_time_hbm, to_time))
        )
    ]
    for load in small:
        load.start()

    def remote(outgoing, incoming, kind, turn, part, recv, p):
        pltpu.make_async_remote_copy(
            src_ref=outgoing.at[turn, part, p],
            dst_ref=incoming.at[turn, part, me],
            send_sem=send_sem.at[kind, turn, part],
            recv_sem=recv,
            device_id={"freq": p},
            device_id_type=MESH,
        ).start()

    def own(outgoing, incoming, kind, turn, part):
        return pltpu.make_async_copy(
            outgoing.at[turn, part, me], incoming.at[turn, part, me], own_sem.at[kind, turn, part]
        )

    def send_image(turn, part, p):
        remote(image_out, image_in, 0, turn, part, image_sem.at[turn, part], p)

    def image_arrived(turn, part):
        rest = image_in.at[turn, part, pl.ds(0, group - 1)]
        pltpu.make_async_copy(rest, rest, image_sem.at[turn, part]).wait()
        own(image_out, image_in, 0, turn, part).wait()

    def send_spec(turn, part):
        for_peers(
            lambda p: remote(spec_out, spec_in, 1, turn, part, spec_sem.at[turn, part, mine], p)
        )
        own(spec_out, spec_in, 1, turn, part).start()

    def spec_arrived(turn, part, t):
        count = team - 1 if TEAM_ORDER[t] == 0 else team
        rest = spec_in.at[turn, part, pl.ds(0, count)]
        pltpu.make_async_copy(rest, rest, spec_sem.at[turn, part, order[t]]).wait()
        if TEAM_ORDER[t] == 0:
            own(spec_out, spec_in, 1, turn, part).wait()

    def sent(outgoing, kind, turn, part):
        rest = outgoing.at[turn, part, pl.ds(0, group - 1)]
        pltpu.make_async_copy(rest, rest, send_sem.at[kind, turn, part]).wait()

    lane = lax.broadcasted_iota(jnp.int32, (1, 128), 1)

    def row_of(values):
        row = jnp.zeros((1, 128), F32)
        for i, value in enumerate(values):
            row = jnp.where(lane == i, value, row)
        return row

    def mate_copy(slot):
        return pltpu.make_async_remote_copy(
            src_ref=sums_own.at[slot],
            dst_ref=sums_mate.at[slot],
            send_sem=mate_send.at[slot],
            recv_sem=mate_recv.at[slot],
            device_id={"freq": peer(0, 1)},
            device_id_type=MESH,
        )

    def share(slot, values):
        sums_own[slot] = row_of(values)
        mate_copy(slot).start()

    def relay(slot):
        mate_copy(slot).wait()
        row = sums_own[slot] + sums_mate[slot]
        sums_out[slot] = row
        sums_in[slot, chip] = row

        def push(p):
            pltpu.make_async_remote_copy(
                src_ref=sums_out.at[slot],
                dst_ref=sums_in.at[slot, chip],
                send_sem=sum_send.at[slot],
                recv_sem=sum_recv.at[slot],
                device_id={"freq": p},
                device_id_type=MESH,
            ).start()

        push(peer(chips // 2, 0))

        def step(i, carry):
            d = chips // 2 - 1 - i
            push(peer(d, 0))
            push(peer(-d, 0))
            return carry

        lax.fori_loop(0, chips // 2 - 1, step, 0)

    def share_last(slot, value):
        row = row_of((value,))
        sums_out[slot] = row
        last_in[me] = row

        def push(p):
            pltpu.make_async_remote_copy(
                src_ref=sums_out.at[slot],
                dst_ref=last_in.at[me],
                send_sem=sum_send.at[slot],
                recv_sem=sum_recv.at[slot],
                device_id={"freq": p},
                device_id_type=MESH,
            ).start()

        for_peers(push)

    def collect_last(slot):
        sums_wait(slot, sum_recv)
        total = jnp.sum(last_in[...], axis=0)
        return jnp.sum(jnp.where(lane == 0, total, 0.0), axis=1, keepdims=True)

    def sums_wait(slot, sem):
        last = slot == LAST
        rest = last_in.at[pl.ds(0, group - 1)] if last else sums_in.at[slot, pl.ds(0, chips - 1)]
        pltpu.make_async_copy(rest, rest, sem.at[slot]).wait()

    def collect(slot, count):
        sums_wait(slot, sum_recv)
        total = jnp.sum(sums_in[slot], axis=0)
        return [jnp.sum(jnp.where(lane == i, total, 0.0), axis=1, keepdims=True) for i in range(count)]

    def full_sum(values):
        return jnp.sum(jnp.sum(values, axis=0, keepdims=True), axis=1, keepdims=True)

    def put_duals(h, rows, real, imag):
        low = pl.ds(pl.multiple_of(src + rows.start, 128), rows.size)
        duals[h, rows, :focal] = real.astype(BF16)
        duals[h, rows, focal:] = imag.astype(BF16)
        duals[h, low, :focal] = imag.astype(BF16)
        duals[h, low, focal:] = (-real).astype(BF16)

    tile = 256

    def adjoint(turn, t, ready):
        rows = cols_of(t)
        owner = order[t] * team
        for h in range(nf):
            ready(t, h)
            got = dot(kern_t[0, h, rows, :], duals[h, :src, :]) + dot(
                kern_t[1, h, rows, :], duals[h, src:, :]
            )
            real = got[:, :focal].reshape(team, 2, HALF, focal)
            imag = got[:, focal:].reshape(team, 2, HALF, focal)
            for part in range(2):
                image_out[turn, part, pl.ds(owner, team), h] = jnp.concatenate(
                    [real[:, part], imag[:, part]], axis=1
                ).astype(BF16)

    def send_team(turn, t):
        first = 1 if TEAM_ORDER[t] == 0 else 0

        def push(i, carry):
            send_image(turn, 0, order[t] * team + lax.rem(seat + i, team))
            return carry

        lax.fori_loop(first, team, push, 0)

    def send_rest(turn):
        own(image_out, image_in, 0, turn, 0).start()
        for_peers(lambda p: send_image(turn, 1, p))
        own(image_out, image_in, 0, turn, 1).start()

    def row_at(row):
        return pl.ds(row, samples, stride=held)

    def window(turn, part, combine):
        wide[...] = image_in[turn, part].astype(F32).reshape(bins * 2 * HALF, focal)
        norm = jnp.zeros((1, 2 * focal), F32)
        time = lax.broadcasted_iota(jnp.int32, (samples, focal), 0)
        for pair in range(HALF // 2):
            first, second = 2 * pair, 2 * pair + 1

            def column(r):
                return jnp.concatenate(
                    [
                        wide[pl.ds(r, bins, stride=2 * HALF), :],
                        wide[pl.ds(HALF + r, bins, stride=2 * HALF), :],
                    ],
                    axis=0,
                ).astype(BF16)

            timed = dot(to_time[...], jnp.concatenate([column(first), column(second)], axis=1))
            kept = []
            for i, r in enumerate((first, second)):
                row = part * HALF + r
                keep = time < onset[pl.ds(row, 1), :]
                value = jnp.where(keep, timed[:, i * focal : (i + 1) * focal], 0.0)
                kept.append(combine(row, value))
            kept = jnp.concatenate(kept, axis=1)
            norm = norm + jnp.sum(kept * kept, axis=0, keepdims=True)
            spec = dot(to_freq[...], kept.astype(BF16))
            for i, r in enumerate((first, second)):
                cols = slice(i * focal, (i + 1) * focal)
                wide[pl.ds(r, bins, stride=2 * HALF), :] = spec[:bins, cols]
                wide[pl.ds(HALF + r, bins, stride=2 * HALF), :] = spec[bins:, cols]
        spec_out[turn, part] = wide[...].reshape(group, nf, 2 * HALF, focal).astype(BF16)
        return norm

    def forward(turn, finish):
        norm = jnp.zeros((1, 2 * focal), F32)
        for t in range(TEAMS):
            for part in range(2):
                spec_arrived(turn, part, t)
            for h in range(nf):
                blocks = [
                    spec_in[turn, part, pl.ds(order[t] * team, team), h].astype(F32)
                    for part in range(2)
                ]
                real = jnp.concatenate([b[:, :HALF] for b in blocks], axis=1).reshape(block, focal)
                imag = jnp.concatenate([b[:, HALF:] for b in blocks], axis=1).reshape(block, focal)
                weights[h, 0, :, :focal] = real.astype(BF16)
                weights[h, 0, :, focal:] = imag.astype(BF16)
                weights[h, 1, :, :focal] = (-imag).astype(BF16)
                weights[h, 1, :, focal:] = real.astype(BF16)

                def step(i, norm):
                    rows = pl.ds(pl.multiple_of(i * TALL, TALL), TALL)
                    got = dot(kern[0, h, rows, cols_of(t)], weights[h, 0]) + dot(
                        kern[1, h, rows, cols_of(t)], weights[h, 1]
                    )
                    if t > 0:
                        got = got + partial[h, rows, :]
                    if t < TEAMS - 1:
                        partial[h, rows, :] = got
                        return norm
                    value = finish(h, rows, got)
                    return norm + jnp.sum(value * value, axis=0, keepdims=True)

                norm = lax.fori_loop(0, src // TALL, step, norm)
        return full_sum(norm)

    for h in range(nf):
        for c in range(2):
            data_load(c, h).wait()
        put_duals(h, pl.ds(0, src), data[0, h], data[1, h])

    def turn_block(t, h):
        for c in range(2):
            kern_load(t, c, h).wait()

            def flip(i, carry):
                at = pl.ds(pl.multiple_of(i * tile, tile), tile)
                kern_t[c, h, cols_of(t), at] = kern[c, h, at, cols_of(t)].T
                return carry

            lax.fori_loop(0, src // tile, flip, 0)

    for t in range(TEAMS):
        adjoint(0, t, turn_block)
        if t == 0:
            pl.semaphore_wait(barrier, group - 1)
        send_team(0, t)
    send_rest(0)
    data_norm = jnp.zeros((1, focal), F32)
    for h in range(nf):
        for c in range(2):
            data_norm = data_norm + jnp.sum(data[c, h] * data[c, h], axis=0, keepdims=True)
    data_norm = full_sum(data_norm)

    for load in small:
        load.wait()
    norms = []
    for part in range(2):
        image_arrived(0, part)

        def keep_model(row, value):
            model[row_at(row), :] = value
            return value

        norms.append(window(0, part, keep_model))
        if part == 1:
            share(0, (data_norm, full_sum(norms[0] + norms[1])))
            relay(0)
        send_spec(0, part)
    save_model = pltpu.make_async_copy(model, model_hbm, save_sem.at[0])
    save_model.start()

    square_data, square_model = collect(0, 2)
    beta0 = jnp.sqrt(square_data)
    size0 = jnp.sqrt(square_model)
    alpha0 = size0 / beta0
    gain = 1.0 / size0
    back = alpha0 / beta0

    def first_resid(h, rows, got):
        real = got[:, :focal] * gain - back * data[0, h, rows, :]
        imag = got[:, focal:] * gain - back * data[1, h, rows, :]
        put_duals(h, rows, real, imag)
        value = jnp.concatenate([real, imag], axis=1)
        resid[h, rows, :] = value
        return value

    resid_square = forward(0, first_resid)
    share(1, (resid_square,))
    for t in range(TEAMS):
        adjoint(1, t, lambda t, h: None)
        send_team(1, t)
        if t == 0:
            relay(1)
    send_rest(1)

    (square1,) = collect(1, 1)
    beta1 = jnp.sqrt(square1)
    scale1 = 1.0 / beta1
    back1 = beta1 / size0
    norms = []
    for part in range(2):
        image_arrived(1, part)

        def subtract(row, value):
            value = value * scale1 - back1 * model[row_at(row), :]
            field[row_at(row), :] = value
            return value

        norms.append(window(1, part, subtract))
        if part == 1:
            share(2, (full_sum(norms[0] + norms[1]),))
            relay(2)
        send_spec(1, part)
    save_field = pltpu.make_async_copy(field, field_hbm, save_sem.at[1])
    save_field.start()

    (square2,) = collect(2, 1)
    alpha1 = jnp.sqrt(square2)
    gain2 = 1.0 / alpha1
    back2 = alpha1 / beta1

    def second_resid(h, rows, got):
        return got * gain2 - back2 * resid[h, rows, :]

    last_square = forward(1, second_resid)
    share_last(LAST, last_square)
    save_model.wait()
    save_field.wait()
    for turn in range(2):
        for part in range(2):
            sent(image_out, 0, turn, part)
            sent(spec_out, 1, turn, part)
    for slot in range(LAST + 1):
        sums_wait(slot, sum_send)
    beta2 = jnp.sqrt(collect_last(LAST))
    rho1 = jnp.sqrt(alpha0 * alpha0 + beta1 * beta1)
    cosine = alpha0 / rho1
    sine = beta1 / rho1
    theta = sine * alpha1
    rhobar = -cosine * alpha1
    phi1 = cosine * beta0
    phibar = sine * beta0
    rho2 = jnp.sqrt(rhobar * rhobar + beta2 * beta2)
    phi2 = rhobar / rho2 * phibar
    step2 = phi2 / rho2
    on_field[...] = jnp.broadcast_to(step2 / alpha1, on_field.shape)
    on_model[...] = jnp.broadcast_to(
        (phi1 / rho1 - step2 * (theta / rho1)) / size0, on_model.shape
    )


def solution(mesh):
    group = mesh.shape["freq"]

    def shard(kernel, recorded, onset_time):
        nf, src, rec = kernel.shape[1:]
        held, focal = onset_time.shape
        bins = group * nf
        samples = 2 * bins
        forth = dft_tables(bins)
        moved = (2, 2, group, nf, 2 * HALF, focal)
        flat = (samples * held, focal)
        dma = pltpu.SemaphoreType.DMA
        anywhere = pl.BlockSpec(memory_space=pl.ANY)
        vmem = pl.BlockSpec(memory_space=pltpu.VMEM)
        model, field, on_model, on_field = pl.pallas_call(
            functools.partial(body, group),
            out_shape=(
                pltpu.VMEM(flat, F32),
                pltpu.VMEM(flat, F32),
                pltpu.VMEM((1, focal), F32),
                pltpu.VMEM((1, focal), F32),
            ),
            in_specs=[pl.BlockSpec(memory_space=pltpu.HBM)] * 5,
            out_specs=(anywhere, anywhere, vmem, vmem),
            scratch_shapes=[
                pltpu.VMEM(onset_time.shape, jnp.int32),
                pltpu.VMEM(forth.shape, BF16),
                pltpu.VMEM(forth.shape[::-1], BF16),
                pltpu.VMEM(kernel.shape, BF16),
                pltpu.VMEM((2, nf, rec, src), BF16),
                pltpu.VMEM(recorded.shape, F32),
                pltpu.VMEM((nf, src, 2 * focal), F32),
                pltpu.VMEM((nf, 2 * src, 2 * focal), BF16),
                pltpu.VMEM((nf, 2, rec // TEAMS, 2 * focal), BF16),
                pltpu.VMEM((nf, src, 2 * focal), F32),
                pltpu.VMEM(flat, F32),
                pltpu.VMEM(flat, F32),
                pltpu.VMEM(moved, BF16),
                pltpu.VMEM(moved, BF16),
                pltpu.VMEM(moved, BF16),
                pltpu.VMEM(moved, BF16),
                pltpu.VMEM((bins * 2 * HALF, focal), F32),
                pltpu.VMEM((LAST, 1, 128), F32),
                pltpu.VMEM((LAST, 1, 128), F32),
                pltpu.VMEM((LAST + 1, 1, 128), F32),
                pltpu.VMEM((LAST, group // CORES, 1, 128), F32),
                pltpu.VMEM((group, 1, 128), F32),
                dma((3,)),
                dma((2, nf)),
                dma((TEAMS, 2, nf)),
                dma((2, 2, 2)),
                dma((2, 2)),
                dma((2, 2, TEAMS)),
                dma((2, 2, 2)),
                dma((LAST,)),
                dma((LAST,)),
                dma((LAST + 1,)),
                dma((LAST + 1,)),
                dma((2,)),
            ],
            compiler_params=pltpu.CompilerParams(
                collective_id=0, has_side_effects=True, vmem_limit_bytes=LIMIT * MIB
            ),
        )(kernel, recorded, onset_time, jnp.asarray(forth), jnp.asarray(np.ascontiguousarray(forth.T)))
        x = on_model * model + on_field * field
        return x.reshape(samples, held, focal)

    placed = (
        P(None, ("grp", "freq"), None, None),
        P(None, ("grp", "freq"), None, None),
        P(("grp", "freq"), None),
    )
    return jax.shard_map(
        shard, mesh=mesh, in_specs=placed, out_specs=P(None, ("grp", "freq"), None), check_vma=False
    )
```

```python
import functools

import jax
import jax.numpy as jnp
import numpy as np
from jax import lax
from jax.experimental import pallas as pl
from jax.experimental.pallas import tpu as pltpu
from jax.sharding import PartitionSpec as P

CORES = 2
HALF = 8
MIB = 2**20
TEAMS = 4
TEAM_ORDER = (2, 1, 3, 0)
LIMIT = 58
TALL = 512
LAST = 3
MESH = pl.DeviceIdType.MESH
F32 = jnp.float32
BF16 = jnp.bfloat16


def dft_tables(bins):
    samples = 2 * bins
    phase = np.outer(np.arange(bins), np.arange(samples)) % samples * (np.pi / bins)
    scale = 1.0 / np.sqrt(bins)
    both = np.concatenate([np.cos(phase) * scale, -np.sin(phase) * scale], axis=0)
    return both.astype(jnp.bfloat16)


def dot(left, right):
    return jnp.dot(left, right, preferred_element_type=F32)


def body(
    group,
    kern_hbm,
    data_hbm,
    onset_hbm,
    to_freq_hbm,
    to_time_hbm,
    model_hbm,
    field_hbm,
    on_model,
    on_field,
    onset,
    to_freq,
    to_time,
    kern,
    kern_t,
    data,
    resid,
    duals,
    weights,
    partial,
    model,
    field,
    image_out,
    image_in,
    spec_out,
    spec_in,
    wide,
    sums_own,
    sums_mate,
    sums_out,
    sums_in,
    last_in,
    small_sem,
    data_sem,
    kern_sem,
    send_sem,
    image_sem,
    spec_sem,
    own_sem,
    mate_send,
    mate_recv,
    sum_send,
    sum_recv,
    save_sem,
):
    me = lax.axis_index("freq")
    chips = group // CORES
    chip = me // CORES
    core = lax.rem(me, CORES)
    nf = kern.shape[1]
    src = kern.shape[2]
    held, focal = onset.shape
    bins = group * nf
    samples = 2 * bins
    team = group // TEAMS
    mine = me // team
    seat = lax.rem(me, team)
    block = team * held
    order = [lax.rem(mine + i, TEAMS) for i in TEAM_ORDER]

    def peer(chip_step, core_step):
        return lax.rem(chip + chip_step + chips, chips) * CORES + lax.rem(core + core_step, CORES)

    def for_peers(act):
        far = chips // 2
        for other in range(CORES):
            act(peer(far, other))

        def step(i, carry):
            d = far - 1 - i
            for other in range(CORES):
                act(peer(d, other))
                act(peer(-d, other))
            return carry

        lax.fori_loop(0, far - 1, step, 0)
        act(peer(0, 1))

    def cols_of(t):
        return pl.ds(pl.multiple_of(order[t] * block, block), block)

    def data_load(c, h):
        return pltpu.make_async_copy(data_hbm.at[c, h], data.at[c, h], data_sem.at[c, h])

    def kern_load(t, c, h):
        where = (c, h, slice(None), cols_of(t))
        return pltpu.make_async_copy(kern_hbm.at[where], kern.at[where], kern_sem.at[t, c, h])

    for h in range(nf):
        for c in range(2):
            data_load(c, h).start()
    for h in range(nf):
        for c in range(2):
            kern_load(0, c, h).start()
    barrier = pltpu.get_barrier_semaphore()
    for_peers(
        lambda p: pl.semaphore_signal(barrier, inc=1, device_id={"freq": p}, device_id_type=MESH)
    )
    for t in range(1, TEAMS):
        for h in range(nf):
            for c in range(2):
                kern_load(t, c, h).start()
    small = [
        pltpu.make_async_copy(source, target, small_sem.at[i])
        for i, (source, target) in enumerate(
            ((onset_hbm, onset), (to_freq_hbm, to_freq), (to_time_hbm, to_time))
        )
    ]
    for load in small:
        load.start()

    def remote(outgoing, incoming, kind, turn, part, recv, p):
        pltpu.make_async_remote_copy(
            src_ref=outgoing.at[turn, part, p],
            dst_ref=incoming.at[turn, part, me],
            send_sem=send_sem.at[kind, turn, part],
            recv_sem=recv,
            device_id={"freq": p},
            device_id_type=MESH,
        ).start()

    def own(outgoing, incoming, kind, turn, part):
        return pltpu.make_async_copy(
            outgoing.at[turn, part, me], incoming.at[turn, part, me], own_sem.at[kind, turn, part]
        )

    def send_image(turn, part, p):
        remote(image_out, image_in, 0, turn, part, image_sem.at[turn, part], p)

    def image_arrived(turn, part):
        rest = image_in.at[turn, part, pl.ds(0, group - 1)]
        pltpu.make_async_copy(rest, rest, image_sem.at[turn, part]).wait()
        own(image_out, image_in, 0, turn, part).wait()

    def send_spec(turn, part):
        for_peers(
            lambda p: remote(spec_out, spec_in, 1, turn, part, spec_sem.at[turn, part, mine], p)
        )
        own(spec_out, spec_in, 1, turn, part).start()

    def spec_arrived(turn, part, t):
        count = team - 1 if TEAM_ORDER[t] == 0 else team
        rest = spec_in.at[turn, part, pl.ds(0, count)]
        pltpu.make_async_copy(rest, rest, spec_sem.at[turn, part, order[t]]).wait()
        if TEAM_ORDER[t] == 0:
            own(spec_out, spec_in, 1, turn, part).wait()

    def sent(outgoing, kind, turn, part):
        rest = outgoing.at[turn, part, pl.ds(0, group - 1)]
        pltpu.make_async_copy(rest, rest, send_sem.at[kind, turn, part]).wait()

    lane = lax.broadcasted_iota(jnp.int32, (1, 128), 1)

    def row_of(values):
        row = jnp.zeros((1, 128), F32)
        for i, value in enumerate(values):
            row = jnp.where(lane == i, value, row)
        return row

    def mate_copy(stage, slot):
        return pltpu.make_async_remote_copy(
            src_ref=sums_own.at[stage, slot],
            dst_ref=sums_mate.at[stage, slot],
            send_sem=mate_send.at[stage, slot],
            recv_sem=mate_recv.at[stage, slot],
            device_id={"freq": peer(0, 1)},
            device_id_type=MESH,
        )

    def share(slot, values):
        sums_own[0, slot] = row_of(values)
        mate_copy(0, slot).start()

    far = chips // 2

    def relay(slot):
        mate_copy(0, slot).wait()
        sums_out[slot] = sums_own[0, slot] + sums_mate[0, slot]

        def step(i, carry):
            pltpu.make_async_remote_copy(
                src_ref=sums_out.at[slot],
                dst_ref=sums_in.at[slot, i],
                send_sem=sum_send.at[slot],
                recv_sem=sum_recv.at[slot],
                device_id={"freq": peer((far - i) * (1 - 2 * core), 0)},
                device_id_type=MESH,
            ).start()
            return carry

        lax.fori_loop(0, far, step, 0)

    def share_last(slot, value):
        row = row_of((value,))
        sums_out[slot] = row
        last_in[me] = row

        def push(p):
            pltpu.make_async_remote_copy(
                src_ref=sums_out.at[slot],
                dst_ref=last_in.at[me],
                send_sem=sum_send.at[slot],
                recv_sem=sum_recv.at[slot],
                device_id={"freq": p},
                device_id_type=MESH,
            ).start()

        for_peers(push)

    def collect_last(slot):
        sums_wait(slot, sum_recv)
        total = jnp.sum(last_in[...], axis=0)
        return jnp.sum(jnp.where(lane == 0, total, 0.0), axis=1, keepdims=True)

    def sums_wait(slot, sem):
        last = slot == LAST
        rest = last_in.at[pl.ds(0, group - 1)] if last else sums_in.at[slot]
        pltpu.make_async_copy(rest, rest, sem.at[slot]).wait()

    def collect(slot, count):
        sums_wait(slot, sum_recv)
        once = (1 - core).astype(F32) * (sums_in[slot, 0] + sums_out[slot])
        sums_own[1, slot] = once + jnp.sum(sums_in[slot, 1:far], axis=0)
        mate_copy(1, slot).start()
        mate_copy(1, slot).wait()
        total = sums_own[1, slot] + sums_mate[1, slot]
        return [jnp.sum(jnp.where(lane == i, total, 0.0), axis=1, keepdims=True) for i in range(count)]

    def full_sum(values):
        return jnp.sum(jnp.sum(values, axis=0, keepdims=True), axis=1, keepdims=True)

    def put_duals(h, rows, real, imag):
        low = pl.ds(pl.multiple_of(src + rows.start, 128), rows.size)
        duals[h, rows, :focal] = real.astype(BF16)
        duals[h, rows, focal:] = imag.astype(BF16)
        duals[h, low, :focal] = imag.astype(BF16)
        duals[h, low, focal:] = (-real).astype(BF16)

    tile = 256

    def adjoint(turn, t, ready):
        rows = cols_of(t)
        owner = order[t] * team
        for h in range(nf):
            ready(t, h)
            got = dot(kern_t[0, h, rows, :], duals[h, :src, :]) + dot(
                kern_t[1, h, rows, :], duals[h, src:, :]
            )
            real = got[:, :focal].reshape(team, 2, HALF, focal)
            imag = got[:, focal:].reshape(team, 2, HALF, focal)
            for part in range(2):
                image_out[turn, part, pl.ds(owner, team), h] = jnp.concatenate(
                    [real[:, part], imag[:, part]], axis=1
                ).astype(BF16)

    def send_team(turn, t):
        first = 1 if TEAM_ORDER[t] == 0 else 0

        def push(i, carry):
            send_image(turn, 0, order[t] * team + lax.rem(seat + i, team))
            return carry

        lax.fori_loop(first, team, push, 0)

    def send_rest(turn):
        own(image_out, image_in, 0, turn, 0).start()
        for_peers(lambda p: send_image(turn, 1, p))
        own(image_out, image_in, 0, turn, 1).start()

    def row_at(row):
        return pl.ds(row, samples, stride=held)

    def window(turn, part, combine):
        wide[...] = image_in[turn, part].astype(F32).reshape(bins * 2 * HALF, focal)
        norm = jnp.zeros((1, 2 * focal), F32)
        time = lax.broadcasted_iota(jnp.int32, (samples, focal), 0)
        for pair in range(HALF // 2):
            first, second = 2 * pair, 2 * pair + 1

            def column(r):
                return jnp.concatenate(
                    [
                        wide[pl.ds(r, bins, stride=2 * HALF), :],
                        wide[pl.ds(HALF + r, bins, stride=2 * HALF), :],
                    ],
                    axis=0,
                ).astype(BF16)

            timed = dot(to_time[...], jnp.concatenate([column(first), column(second)], axis=1))
            kept = []
            for i, r in enumerate((first, second)):
                row = part * HALF + r
                keep = time < onset[pl.ds(row, 1), :]
                value = jnp.where(keep, timed[:, i * focal : (i + 1) * focal], 0.0)
                kept.append(combine(row, value))
            kept = jnp.concatenate(kept, axis=1)
            norm = norm + jnp.sum(kept * kept, axis=0, keepdims=True)
            spec = dot(to_freq[...], kept.astype(BF16))
            for i, r in enumerate((first, second)):
                cols = slice(i * focal, (i + 1) * focal)
                wide[pl.ds(r, bins, stride=2 * HALF), :] = spec[:bins, cols]
                wide[pl.ds(HALF + r, bins, stride=2 * HALF), :] = spec[bins:, cols]
        spec_out[turn, part] = wide[...].reshape(group, nf, 2 * HALF, focal).astype(BF16)
        return norm

    def forward(turn, finish):
        norm = jnp.zeros((1, 2 * focal), F32)
        for t in range(TEAMS):
            for part in range(2):
                spec_arrived(turn, part, t)
            for h in range(nf):
                blocks = [
                    spec_in[turn, part, pl.ds(order[t] * team, team), h].astype(F32)
                    for part in range(2)
                ]
                real = jnp.concatenate([b[:, :HALF] for b in blocks], axis=1).reshape(block, focal)
                imag = jnp.concatenate([b[:, HALF:] for b in blocks], axis=1).reshape(block, focal)
                weights[h, 0, :, :focal] = real.astype(BF16)
                weights[h, 0, :, focal:] = imag.astype(BF16)
                weights[h, 1, :, :focal] = (-imag).astype(BF16)
                weights[h, 1, :, focal:] = real.astype(BF16)

                def step(i, norm):
                    rows = pl.ds(pl.multiple_of(i * TALL, TALL), TALL)
                    got = dot(kern[0, h, rows, cols_of(t)], weights[h, 0]) + dot(
                        kern[1, h, rows, cols_of(t)], weights[h, 1]
                    )
                    if t > 0:
                        got = got + partial[h, rows, :]
                    if t < TEAMS - 1:
                        partial[h, rows, :] = got
                        return norm
                    value = finish(h, rows, got)
                    return norm + jnp.sum(value * value, axis=0, keepdims=True)

                norm = lax.fori_loop(0, src // TALL, step, norm)
        return full_sum(norm)

    for h in range(nf):
        for c in range(2):
            data_load(c, h).wait()
        put_duals(h, pl.ds(0, src), data[0, h], data[1, h])

    def turn_block(t, h):
        for c in range(2):
            kern_load(t, c, h).wait()

            def flip(i, carry):
                at = pl.ds(pl.multiple_of(i * tile, tile), tile)
                kern_t[c, h, cols_of(t), at] = kern[c, h, at, cols_of(t)].T
                return carry

            lax.fori_loop(0, src // tile, flip, 0)

    for t in range(TEAMS):
        adjoint(0, t, turn_block)
        if t == 0:
            pl.semaphore_wait(barrier, group - 1)
        send_team(0, t)
    send_rest(0)
    data_norm = jnp.zeros((1, focal), F32)
    for h in range(nf):
        for c in range(2):
            data_norm = data_norm + jnp.sum(data[c, h] * data[c, h], axis=0, keepdims=True)
    data_norm = full_sum(data_norm)

    for load in small:
        load.wait()
    norms = []
    for part in range(2):
        image_arrived(0, part)

        def keep_model(row, value):
            model[row_at(row), :] = value
            return value

        norms.append(window(0, part, keep_model))
        if part == 1:
            share(0, (data_norm, full_sum(norms[0] + norms[1])))
            relay(0)
        send_spec(0, part)
    save_model = pltpu.make_async_copy(model, model_hbm, save_sem.at[0])
    save_model.start()

    square_data, square_model = collect(0, 2)
    beta0 = jnp.sqrt(square_data)
    size0 = jnp.sqrt(square_model)
    alpha0 = size0 / beta0
    gain = 1.0 / size0
    back = alpha0 / beta0

    def first_resid(h, rows, got):
        real = got[:, :focal] * gain - back * data[0, h, rows, :]
        imag = got[:, focal:] * gain - back * data[1, h, rows, :]
        put_duals(h, rows, real, imag)
        value = jnp.concatenate([real, imag], axis=1)
        resid[h, rows, :] = value
        return value

    resid_square = forward(0, first_resid)
    share(1, (resid_square,))
    for t in range(TEAMS):
        adjoint(1, t, lambda t, h: None)
        send_team(1, t)
        if t == 0:
            relay(1)
    send_rest(1)

    (square1,) = collect(1, 1)
    beta1 = jnp.sqrt(square1)
    scale1 = 1.0 / beta1
    back1 = beta1 / size0
    norms = []
    for part in range(2):
        image_arrived(1, part)

        def subtract(row, value):
            value = value * scale1 - back1 * model[row_at(row), :]
            field[row_at(row), :] = value
            return value

        norms.append(window(1, part, subtract))
        if part == 1:
            share(2, (full_sum(norms[0] + norms[1]),))
            relay(2)
        send_spec(1, part)
    save_field = pltpu.make_async_copy(field, field_hbm, save_sem.at[1])
    save_field.start()

    (square2,) = collect(2, 1)
    alpha1 = jnp.sqrt(square2)
    gain2 = 1.0 / alpha1
    back2 = alpha1 / beta1

    def second_resid(h, rows, got):
        return got * gain2 - back2 * resid[h, rows, :]

    last_square = forward(1, second_resid)
    share_last(LAST, last_square)
    save_model.wait()
    save_field.wait()
    for turn in range(2):
        for part in range(2):
            sent(image_out, 0, turn, part)
            sent(spec_out, 1, turn, part)
    for slot in range(LAST + 1):
        sums_wait(slot, sum_send)
    beta2 = jnp.sqrt(collect_last(LAST))
    rho1 = jnp.sqrt(alpha0 * alpha0 + beta1 * beta1)
    cosine = alpha0 / rho1
    sine = beta1 / rho1
    theta = sine * alpha1
    rhobar = -cosine * alpha1
    phi1 = cosine * beta0
    phibar = sine * beta0
    rho2 = jnp.sqrt(rhobar * rhobar + beta2 * beta2)
    phi2 = rhobar / rho2 * phibar
    step2 = phi2 / rho2
    on_field[...] = jnp.broadcast_to(step2 / alpha1, on_field.shape)
    on_model[...] = jnp.broadcast_to(
        (phi1 / rho1 - step2 * (theta / rho1)) / size0, on_model.shape
    )


def solution(mesh):
    group = mesh.shape["freq"]

    def shard(kernel, recorded, onset_time):
        nf, src, rec = kernel.shape[1:]
        held, focal = onset_time.shape
        bins = group * nf
        samples = 2 * bins
        forth = dft_tables(bins)
        moved = (2, 2, group, nf, 2 * HALF, focal)
        flat = (samples * held, focal)
        dma = pltpu.SemaphoreType.DMA
        anywhere = pl.BlockSpec(memory_space=pl.ANY)
        vmem = pl.BlockSpec(memory_space=pltpu.VMEM)
        model, field, on_model, on_field = pl.pallas_call(
            functools.partial(body, group),
            out_shape=(
                pltpu.VMEM(flat, F32),
                pltpu.VMEM(flat, F32),
                pltpu.VMEM((1, focal), F32),
                pltpu.VMEM((1, focal), F32),
            ),
            in_specs=[pl.BlockSpec(memory_space=pltpu.HBM)] * 5,
            out_specs=(anywhere, anywhere, vmem, vmem),
            scratch_shapes=[
                pltpu.VMEM(onset_time.shape, jnp.int32),
                pltpu.VMEM(forth.shape, BF16),
                pltpu.VMEM(forth.shape[::-1], BF16),
                pltpu.VMEM(kernel.shape, BF16),
                pltpu.VMEM((2, nf, rec, src), BF16),
                pltpu.VMEM(recorded.shape, F32),
                pltpu.VMEM((nf, src, 2 * focal), F32),
                pltpu.VMEM((nf, 2 * src, 2 * focal), BF16),
                pltpu.VMEM((nf, 2, rec // TEAMS, 2 * focal), BF16),
                pltpu.VMEM((nf, src, 2 * focal), F32),
                pltpu.VMEM(flat, F32),
                pltpu.VMEM(flat, F32),
                pltpu.VMEM(moved, BF16),
                pltpu.VMEM(moved, BF16),
                pltpu.VMEM(moved, BF16),
                pltpu.VMEM(moved, BF16),
                pltpu.VMEM((bins * 2 * HALF, focal), F32),
                pltpu.VMEM((2, LAST, 1, 128), F32),
                pltpu.VMEM((2, LAST, 1, 128), F32),
                pltpu.VMEM((LAST + 1, 1, 128), F32),
                pltpu.VMEM((LAST, group // CORES // 2, 1, 128), F32),
                pltpu.VMEM((group, 1, 128), F32),
                dma((3,)),
                dma((2, nf)),
                dma((TEAMS, 2, nf)),
                dma((2, 2, 2)),
                dma((2, 2)),
                dma((2, 2, TEAMS)),
                dma((2, 2, 2)),
                dma((2, LAST)),
                dma((2, LAST)),
                dma((LAST + 1,)),
                dma((LAST + 1,)),
                dma((2,)),
            ],
            compiler_params=pltpu.CompilerParams(
                collective_id=0, has_side_effects=True, vmem_limit_bytes=LIMIT * MIB
            ),
        )(kernel, recorded, onset_time, jnp.asarray(forth), jnp.asarray(np.ascontiguousarray(forth.T)))
        x = on_model * model + on_field * field
        return x.reshape(samples, held, focal)

    placed = (
        P(None, ("grp", "freq"), None, None),
        P(None, ("grp", "freq"), None, None),
        P(("grp", "freq"), None),
    )
    return jax.shard_map(
        shard, mesh=mesh, in_specs=placed, out_specs=P(None, ("grp", "freq"), None), check_vma=False
    )
```
